256 devices in a mesh: gx: 8 (over z), gy: 32 (over x, y, core).
Axes of the slice: x: 4, y: 4, z: 8, core: 2. Of those that a mesh axis runs over, the one named last changes fastest.
Arguments:
- centres: bfloat16 [1048576, 256], P(('gx', 'gy')), may hold values from -20 to 20
- weights: float32 [16, 1048576], P(None, ('gx', 'gy')), may hold values from -0.375 to 0.375
- targets: float32 [16, 2048], P(None, ('gx', 'gy')), may hold values from -6 to 6
- batch_index: int32 [2048], P(('gx', 'gy')), may hold values from 0 to 1048575, as said below
- nystrom_index: int32 [16384], P(('gx', 'gy')), may hold values from 0 to 1048575, as said below
- eigvecs: float32 [16384, 128], P(('gx', 'gy')), may hold values from -0.046875 to 0.046875
- scales: float32 [128], replicated, may hold values from 0.2 to 2
Outputs:
- residual: float32 [16, 2048], P(None, ('gx', 'gy'))
- block_correction: float32 [16, 16384], P(None, ('gx', 'gy'))
The draws below stay inside these ranges and needn't reach their ends.
Inputs may be any that keep to these rules, and one draw needn't show every extreme that they name: `batch_index`: the entries at positions j * 8 to (j + 1) * 8 - 1 name centres j * 4096 to (j + 1) * 4096 - 1, all different. `nystrom_index`: the entries at positions j * 64 to (j + 1) * 64 - 1 name centres j * 4096 to (j + 1) * 4096 - 1, all different.
All inputs are finite; a program needn't handle non-finite values.
Results may differ from the reference program's by a relative error of at most 0.0003.
Values may be sent and summed in bfloat16 or wider, within the bound.
No kernel may reach another device: no remote copies, remote signals or barrier semaphores. Data moves between devices by JAX's collectives and lax.ppermute only.
A program may use at most 192 MiB of HBM per device.

```python
import math
import jax
import jax.numpy as jnp
from jax import lax

D = 256
OUTPUTS = 16
EIGEN = 128
P_DEV = 4096
B_DEV = 8
S_DEV = 64
CENTRES = 1048576
BATCH = 2048
NYSTROM = 16384


def draw_centres(key, part):
    keys = jax.random.split(jax.random.fold_in(key, 11), 6)
    groups = jax.random.randint(keys[0], (CENTRES,), 0, 64)
    mixing = jax.random.normal(keys[1], (16, D), jnp.float32) * 0.25
    latent_noise = jax.random.normal(keys[2], (CENTRES, 16), jnp.float32)
    noise = jnp.clip(jax.random.normal(keys[3], (CENTRES, D), jnp.float32), -5.0, 5.0)
    means = jax.random.normal(keys[4], (64, 16), jnp.float32) * 3.0
    spread = jnp.exp(jax.random.uniform(keys[5], (CENTRES, 1), jnp.float32, jnp.log(0.5), jnp.log(1.5)))
    latent = jnp.take(means, groups, axis=0) + spread * latent_noise
    values = jnp.dot(latent, mixing, precision=lax.Precision.HIGHEST) + noise
    return jnp.clip(values, -20.0, 20.0).astype(jnp.bfloat16)


def index_pair(key):
    device_count = CENTRES // P_DEV
    keys = jax.random.split(jax.random.fold_in(key, 23), device_count)

    def one_device(device_key):
        order = jax.random.permutation(device_key, P_DEV).astype(jnp.int32)
        return (order[:B_DEV], order[B_DEV:B_DEV + S_DEV])
    batch_part, block_part = jax.vmap(one_device)(keys)
    offsets = (jnp.arange(device_count, dtype=jnp.int32) * P_DEV)[:, None]
    return ((batch_part + offsets).reshape(-1), (block_part + offsets).reshape(-1))


def draw_batch_index(key, part):
    return index_pair(key)[0]


def draw_nystrom_index(key, part):
    return index_pair(key)[1]


def levels(stream_key, extent, cuts, low, top_value):
    factor_of = 1.0
    for dim, shards_of in cuts:
        heights = jax.random.uniform(jax.random.fold_in(jax.random.fold_in(stream_key, 6), dim), (shards_of,), jnp.float32, low / len(cuts), top_value / len(cuts))
        factor_of = factor_of * jnp.repeat(jnp.exp(heights), extent[dim] // shards_of).reshape((-1,) + (1,) * (len(extent) - 1 - dim))
    return factor_of


def normal_values(own_key, extent, scale, reach, cuts=(), kind=jnp.bfloat16):
    values = jax.random.normal(own_key, extent, jnp.float32) * scale
    if len(cuts) > 0:
        values = levels(own_key, extent, cuts, -0.22, 0.18) * values
    return jnp.clip(values, min=-reach, max=reach).astype(kind)


def setup_inputs(seed: int = 0) -> dict:
    key_of = jax.random.split(jax.random.key(seed), 8)
    return {
        "centres": draw_centres(jax.random.fold_in(key_of[7], 71), 0),
        "weights": normal_values(key_of[1], (OUTPUTS, CENTRES), (max(CENTRES // 4096, 1)) ** -0.5, 0.375, ((1, 256),), jnp.float32),
        "targets": normal_values(key_of[2], (OUTPUTS, BATCH), 1.0, 6.0, ((1, 256),), jnp.float32),
        "batch_index": draw_batch_index(jax.random.fold_in(key_of[7], 71), 0),
        "nystrom_index": draw_nystrom_index(jax.random.fold_in(key_of[7], 71), 0),
        "eigvecs": normal_values(key_of[5], (NYSTROM, EIGEN), NYSTROM ** -0.5, 0.046875, ((0, 256),), jnp.float32),
        "scales": jnp.clip(jnp.exp(jax.random.uniform(key_of[6], (EIGEN,), jnp.float32, math.log(0.2), math.log(2.0))), 0.2, 2.0),
    }


def kernel_matrix(points, others):
    width = float(points.shape[1]) ** 0.5
    point_norm = lax.optimization_barrier(jnp.sum(points.astype(jnp.float32) ** 2, axis=1))
    other_norm = lax.optimization_barrier(jnp.sum(others.astype(jnp.float32) ** 2, axis=1))
    inner = jnp.dot(points, others.T, preferred_element_type=jnp.float32)
    squared = point_norm[:, None] + other_norm[None, :] - 2.0 * inner
    return jnp.exp(-jnp.sqrt(jnp.maximum(squared, 1.0)) / width)

def reference(centres, weights, targets, batch_index, nystrom_index, eigvecs, scales):
    batch_points = jnp.take(centres, batch_index, axis=0)
    block_count = CENTRES // P_DEV

    def accumulate(step_no, total):
        first = (step_no * P_DEV).astype(jnp.int32)
        others = lax.dynamic_slice_in_dim(centres, first, P_DEV, 0)
        coeffs = lax.dynamic_slice_in_dim(weights, first, P_DEV, 1)
        tile = kernel_matrix(batch_points, others)
        return total + jnp.dot(coeffs, tile.T, precision=lax.Precision.HIGHEST)
    prediction = lax.fori_loop(0, block_count, accumulate, jnp.zeros((OUTPUTS, BATCH), jnp.float32))
    residual = prediction - targets
    block_points = jnp.take(centres, nystrom_index, axis=0)
    block_kernel = kernel_matrix(block_points, batch_points)
    along = jnp.dot(block_kernel, residual.T, precision=lax.Precision.HIGHEST)
    projection = jnp.dot(eigvecs.T, along, precision=lax.Precision.HIGHEST)
    correction = jnp.dot(eigvecs * scales[None, :], projection, precision=lax.Precision.HIGHEST)
    return (residual, correction.T)
```

```python
import math

import jax
import jax.numpy as jnp
from jax import lax
from jax.experimental import pallas as pl
from jax.experimental.pallas import tpu as pltpu
from jax.sharding import Mesh
from jax.sharding import PartitionSpec as P

ALL = ("z", "x", "y", "c")
PLANE = ("x", "y")
COLUMN = ("z", "c")
CHUNK = 256
NT = (((1,), (1,)), ((), ()))
NN = (((1,), (0,)), ((), ()))
VMEM_LIMIT = 48 * 1024 * 1024


def split(v):
    hi = v.astype(jnp.bfloat16)
    lo = (v - hi.astype(jnp.float32)).astype(jnp.bfloat16)
    return hi, lo


def mxu(a, b, dims):
    return lax.dot_general(a, b, dims, preferred_element_type=jnp.float32)


def dot_f32(a, b, dims):
    rows = a.shape[0]
    both = jnp.concatenate(split(a), axis=0)
    b_hi, b_lo = split(b)
    out = mxu(both, b_hi, dims) + mxu(both, b_lo, dims)
    return out[:rows] + out[rows:]


def squares(v):
    wide = v.astype(jnp.float32)
    return split(wide * wide)


def pick_kernel(first_ref, batch_ref, block_ref, centres_ref, rows_ref, points_ref):
    count = centres_ref.shape[0]
    first = first_ref[0]
    sub = lax.broadcasted_iota(jnp.int32, (8, 128), 0)
    lane = lax.broadcasted_iota(jnp.int32, (8, 128), 1)

    def wanted(ref, start):
        tile = jnp.zeros((8, 128), jnp.int32)
        for r in range(8):
            tile = jnp.where(sub == r, ref[start + r] - first, tile)
        return tile

    groups = [wanted(batch_ref, 0)]
    for start in range(0, block_ref.shape[0], 8):
        groups.append(wanted(block_ref, start))
    found = jnp.zeros((8 * len(groups), centres_ref.shape[1]), jnp.float32)
    for base in range(0, count, CHUNK):
        pieces = []
        for tile in groups:
            halves = [
                jnp.where(tile == lane + (base + k), 1.0, 0.0) for k in range(0, CHUNK, 128)
            ]
            pieces.append(jnp.concatenate(halves, axis=1))
        hot = jnp.concatenate(pieces, axis=0).astype(jnp.bfloat16)
        found = found + mxu(hot, centres_ref[base : base + CHUNK, :], NN)
    batch = found[:8].astype(jnp.bfloat16)
    rows_ref[...] = jnp.broadcast_to(batch[None], rows_ref.shape)
    points_ref[...] = found[8:].astype(jnp.bfloat16)


def prepare_kernel(centres_ref, points_ref, weights_ref, norm_ref, point_norm_ref, terms_ref):
    ones = jnp.ones((centres_ref.shape[1], 128), jnp.bfloat16)

    def norms(v):
        hi, lo = squares(v)
        return mxu(hi, ones, NN) + mxu(lo, ones, NN)

    for base in range(0, centres_ref.shape[0], CHUNK):
        norm_ref[base : base + CHUNK, :] = norms(centres_ref[base : base + CHUNK, :])
    point_norm_ref[...] = norms(points_ref[...])
    terms_ref[...] = jnp.concatenate(split(weights_ref[...]), axis=0)


def tile_kernel(
    core_ref, own_ref, other_ref, centres_ref, norm_ref, terms_ref, points_ref, point_norm_ref,
    out_ref, block_hi_ref, block_lo_ref,
):
    depth = centres_ref.shape[1]
    pieces = []
    for h in range(2):
        pieces.append(own_ref[:, h].reshape(-1, depth))
        pieces.append(other_ref[:, h].reshape(-1, depth))
    rows = jnp.concatenate(pieces, axis=0)
    hi, lo = squares(rows)
    ones = jnp.ones((8, depth), jnp.bfloat16)
    row_norm = (mxu(ones, hi, NT) + mxu(ones, lo, NT))[:1]
    doubled = rows * jnp.bfloat16(-2.0)
    factor = -1.0 / (float(depth) ** 0.5 * math.log(2.0))

    def kernel_values(v, v_norm):
        inner = mxu(v, doubled, NT)
        wide = jnp.concatenate([v_norm, v_norm], axis=1)
        squared = jnp.maximum((wide + row_norm) + inner, 1.0)
        return jnp.exp2(squared * lax.rsqrt(squared) * factor)

    total = jnp.zeros((terms_ref.shape[0], rows.shape[0]), jnp.float32)
    for base in range(0, centres_ref.shape[0], CHUNK):
        values = kernel_values(
            centres_ref[base : base + CHUNK, :], norm_ref[base : base + CHUNK, :]
        )
        k_hi, k_lo = split(values)
        terms = terms_ref[:, base : base + CHUNK]
        total = total + mxu(terms, k_hi, NN)
        total = total + mxu(terms, k_lo, NN)
    outputs = total.shape[0] // 2
    predicted = total[:outputs] + total[outputs:]
    block = kernel_values(points_ref[...], point_norm_ref[...])
    swapped = core_ref[0] == 1

    def ordered(v):
        return jnp.where(swapped, pltpu.roll(v, 64, 1), v)

    for h in range(2):
        out_ref[h] = ordered(predicted[:, h * 128 : (h + 1) * 128])
        b_hi, b_lo = split(ordered(block[:, h * 128 : (h + 1) * 128]))
        block_hi_ref[:, h * 128 : (h + 1) * 128] = b_hi
        block_lo_ref[:, h * 128 : (h + 1) * 128] = b_lo


def combine_kernel(parts_ref, less_ref, out_ref):
    total = jnp.sum(parts_ref[...], axis=0) - less_ref[...]
    out_ref[...] = jnp.broadcast_to(total[None], out_ref.shape)


def spread_kernel(parts_ref, out_ref):
    total = jnp.sum(parts_ref[...], axis=0)
    out_ref[...] = jnp.broadcast_to(total[None], out_ref.shape)


def project_kernel(residual_ref, block_hi_ref, block_lo_ref, vectors_ref, out_ref):
    residual = jnp.concatenate([residual_ref[h] for h in range(residual_ref.shape[0])], axis=1)
    rows = residual.shape[0]
    both = jnp.concatenate(split(residual), axis=0)
    along = mxu(both, block_hi_ref[...], NT) + mxu(both, block_lo_ref[...], NT)
    along = along[:rows] + along[rows:]
    projection = dot_f32(along, vectors_ref[...], NN)
    out_ref[...] = jnp.broadcast_to(projection[None], out_ref.shape)


def correct_kernel(parts_ref, scales_ref, vectors_ref, out_ref):
    projection = jnp.sum(parts_ref[...], axis=0) * scales_ref[...]
    out_ref[...] = dot_f32(projection, vectors_ref[...], NT)


def call(kernel, out, *args, **kwargs):
    return pl.pallas_call(
        kernel,
        out_shape=out,
        compiler_params=pltpu.CompilerParams(vmem_limit_bytes=VMEM_LIMIT),
        **kwargs,
    )(*args)


def shape(dims, dtype=jnp.float32):
    return jax.ShapeDtypeStruct(dims, dtype)


def exchange(x, axes):
    return lax.all_to_all(x, axes, split_axis=0, concat_axis=0, tiled=True)


def on_device(centres, weights, targets, batch_index, nystrom_index, eigvecs, scales):
    count, depth = centres.shape
    outputs = weights.shape[0]
    own = batch_index.shape[0]
    block = nystrom_index.shape[0]
    sizes = {a: lax.axis_size(a) for a in ALL}
    plane = sizes["x"] * sizes["y"]
    chips = sizes["z"] * plane
    column = sizes["z"] * sizes["c"]
    first = (lax.axis_index(ALL) * count).astype(jnp.int32).reshape(1)
    core = lax.axis_index("c").astype(jnp.int32).reshape(1)
    place = lax.axis_index("c") * sizes["z"] + lax.axis_index("z")
    smem = pl.BlockSpec(memory_space=pltpu.SMEM)
    vmem = pl.BlockSpec(memory_space=pltpu.VMEM)

    rows, points = call(
        pick_kernel,
        (shape((chips, own, depth), jnp.bfloat16), shape((block, depth), jnp.bfloat16)),
        first, batch_index, nystrom_index, centres,
        in_specs=[smem, smem, smem, vmem],
        out_specs=(vmem, vmem),
    )
    mine = exchange(rows, ("z", "x", "y")).reshape(sizes["z"], plane, own, depth)
    norm, point_norm, terms = call(
        prepare_kernel,
        (shape((count, 128)), shape((block, 128)), shape((2 * outputs, count), jnp.bfloat16)),
        centres, points, weights,
    )
    other = lax.ppermute(mine, "c", [(0, 1), (1, 0)])

    whole = lambda *dims: pl.BlockSpec(dims, lambda i: (0,) * len(dims))
    rows_spec = pl.BlockSpec((sizes["z"], 2, own, depth), lambda i: (0, i, 0, 0))
    batch = plane * 128
    predicted, block_hi, block_lo = call(
        tile_kernel,
        (
            shape((plane, outputs, 128)),
            shape((block, batch), jnp.bfloat16),
            shape((block, batch), jnp.bfloat16),
        ),
        core, mine, other, centres, norm, terms, points, point_norm,
        grid=(plane // 2,),
        in_specs=[
            smem, rows_spec, rows_spec, whole(count, depth), whole(count, 128),
            whole(2 * outputs, count), whole(block, depth), whole(block, 128),
        ],
        out_specs=(
            pl.BlockSpec((2, outputs, 128), lambda i: (i, 0, 0)),
            pl.BlockSpec((block, 256), lambda i: (0, i)),
            pl.BlockSpec((block, 256), lambda i: (0, i)),
        ),
    )
    lanes = lax.broadcasted_iota(jnp.int32, (outputs, 128), 1) // own
    less = jnp.where(lanes == place, jnp.tile(targets, (1, 128 // own)), 0.0)
    gathered = exchange(predicted, PLANE)
    summed = call(combine_kernel, shape((column, outputs, 128)), gathered, less)
    summed = exchange(summed, COLUMN)
    residual = call(spread_kernel, shape((plane, outputs, 128)), summed)
    residual_local = lax.dynamic_slice(residual, (0, 0, place * own), (1, outputs, own))[0]
    residual = exchange(residual, PLANE)
    projection = call(
        project_kernel, shape((plane, outputs, 128)), residual, block_hi, block_lo, eigvecs
    )
    projection = exchange(projection, PLANE)
    projection = call(spread_kernel, shape((column, outputs, 128)), projection)
    projection = exchange(projection, COLUMN)
    correction = call(
        correct_kernel, shape((outputs, block)), projection, scales[None, :], eigvecs
    )
    return residual_local, correction


def solution(mesh):
    finer = Mesh(mesh.devices.reshape(mesh.shape["gx"], 4, 4, 2), ALL)
    in_specs = (
        P(ALL, None),
        P(None, ALL),
        P(None, ALL),
        P(ALL),
        P(ALL),
        P(ALL, None),
        P(),
    )
    out_specs = (P(None, ALL), P(None, ALL))
    return jax.shard_map(
        on_device, mesh=finer, in_specs=in_specs, out_specs=out_specs, check_vma=False
    )
```

```python
import math

import jax
import jax.numpy as jnp
from jax import lax
from jax.experimental import pallas as pl
from jax.experimental.pallas import tpu as pltpu
from jax.sharding import Mesh
from jax.sharding import PartitionSpec as P

ALL = ("z", "x", "y", "c")
PLANE = ("x", "y")
COLUMN = ("z", "c")
CHUNK = 256
NT = (((1,), (1,)), ((), ()))
NN = (((1,), (0,)), ((), ()))
VMEM_LIMIT = 24 * 1024 * 1024


def split(v):
    hi = v.astype(jnp.bfloat16)
    lo = (v - hi.astype(jnp.float32)).astype(jnp.bfloat16)
    return hi, lo


def mxu(a, b, dims):
    return lax.dot_general(a, b, dims, preferred_element_type=jnp.float32)


def dot_f32(a, b, dims):
    rows = a.shape[0]
    both = jnp.concatenate(split(a), axis=0)
    b_hi, b_lo = split(b)
    out = mxu(both, b_hi, dims) + mxu(both, b_lo, dims)
    return out[:rows] + out[rows:]


def squares(v):
    wide = v.astype(jnp.float32)
    return split(wide * wide)


def pick_kernel(first_ref, batch_ref, centres_ref, rows_ref, index_ref, tiles_ref, index_sem, sems):
    own = batch_ref.shape[0]
    fetch = pltpu.make_async_copy(batch_ref, index_ref, index_sem)
    fetch.start()
    fetch.wait()
    first = first_ref[0]
    copies = []
    for r in range(own):
        row = index_ref[r] - first
        base = pl.multiple_of((row // 8) * 8, 8)
        copy = pltpu.make_async_copy(
            centres_ref.at[pl.ds(base, 8), :], tiles_ref.at[r], sems.at[r]
        )
        copy.start()
        copies.append(copy)
    sub = lax.broadcasted_iota(jnp.int32, tiles_ref.shape[1:], 0)
    picked = jnp.zeros(tiles_ref.shape[1:], jnp.float32)
    for r, copy in enumerate(copies):
        copy.wait()
        wanted = (index_ref[r] - first) % 8
        tile = jnp.where(sub == wanted, tiles_ref[r].astype(jnp.float32), 0.0)
        picked = jnp.where(sub == r, jnp.sum(tile, axis=0, keepdims=True), picked)
    rows_ref[...] = jnp.broadcast_to(picked.astype(jnp.bfloat16)[None], rows_ref.shape)


def prepare_kernel(
    first_ref, block_ref, centres_ref, weights_ref,
    norm_ref, points_ref, point_norm_ref, hi_ref, lo_ref, index_ref, index_sem,
):
    fetch = pltpu.make_async_copy(block_ref, index_ref, index_sem)
    fetch.start()
    ones = jnp.ones((centres_ref.shape[1], 128), jnp.bfloat16)

    def norms(v):
        hi, lo = squares(v)
        return mxu(hi, ones, NN) + mxu(lo, ones, NN)

    hi, lo = split(weights_ref[...])
    hi_ref[...] = hi
    lo_ref[...] = lo
    fetch.wait()
    first = first_ref[0]
    sub = lax.broadcasted_iota(jnp.int32, (8, 128), 0)
    lane = lax.broadcasted_iota(jnp.int32, (8, 128), 1)
    groups = []
    for start in range(0, points_ref.shape[0], 8):
        tile = jnp.zeros((8, 128), jnp.int32)
        for r in range(8):
            tile = jnp.where(sub == r, index_ref[start + r] - first, tile)
        groups.append(tile)
    found = jnp.zeros(points_ref.shape, jnp.float32)
    for base in range(0, centres_ref.shape[0], 256):
        centres = centres_ref[base : base + 256, :]
        norm_ref[base : base + 256, :] = norms(centres)
        pieces = []
        for tile in groups:
            halves = [jnp.where(tile == lane + (base + k), 1.0, 0.0) for k in (0, 128)]
            pieces.append(jnp.concatenate(halves, axis=1))
        hot = jnp.concatenate(pieces, axis=0).astype(jnp.bfloat16)
        found = found + mxu(hot, centres, NN)
    points = found.astype(jnp.bfloat16)
    points_ref[...] = points
    point_norm_ref[...] = norms(points)


def tile_kernel(
    core_ref, own_ref, other_ref, centres_ref, norm_ref, hi_ref, lo_ref, points_ref,
    point_norm_ref, out_ref, block_hi_ref, block_lo_ref,
):
    depth = centres_ref.shape[1]
    rows = jnp.concatenate([own_ref[0], other_ref[0], own_ref[1], other_ref[1]], axis=0)
    hi, lo = squares(rows)
    ones = jnp.ones((8, depth), jnp.bfloat16)
    row_norm = (mxu(ones, hi, NT) + mxu(ones, lo, NT))[:1]
    doubled = rows * jnp.bfloat16(-2.0)
    factor = -1.0 / (float(depth) ** 0.5 * math.log(2.0))

    def kernel_values(v, v_norm):
        wide = jnp.concatenate([v_norm, v_norm], axis=1)
        squared = jnp.maximum((wide + row_norm) + mxu(v, doubled, NT), 1.0)
        return jnp.exp2(squared * lax.rsqrt(squared) * factor)

    both_terms = jnp.concatenate([hi_ref[...], lo_ref[...]], axis=0)
    outputs = hi_ref.shape[0]
    total = jnp.zeros((2 * outputs, rows.shape[0]), jnp.float32)
    for base in range(0, centres_ref.shape[0], CHUNK):
        values = kernel_values(
            centres_ref[base : base + CHUNK, :], norm_ref[base : base + CHUNK, :]
        )
        k_hi = values.astype(jnp.bfloat16)
        rest = values - k_hi.astype(jnp.float32)
        terms = both_terms[:, base : base + CHUNK]
        total = total + mxu(terms, k_hi, NN)
        total = total + mxu(terms, rest.astype(jnp.bfloat16), NN)
    predicted = total[:outputs] + total[outputs:]
    block = kernel_values(points_ref[...], point_norm_ref[...])
    swapped = core_ref[0] == 1

    def ordered(v):
        return jnp.where(swapped, pltpu.roll(v, 64, 1), v)

    for h in range(2):
        out_ref[h] = ordered(predicted[:, h * 128 : (h + 1) * 128])
        b_hi, b_lo = split(ordered(block[:, h * 128 : (h + 1) * 128]))
        block_hi_ref[:, h * 128 : (h + 1) * 128] = b_hi
        block_lo_ref[:, h * 128 : (h + 1) * 128] = b_lo


def combine_kernel(parts_ref, less_ref, out_ref):
    total = jnp.sum(parts_ref[...], axis=0) - less_ref[...]
    out_ref[...] = jnp.broadcast_to(total[None], out_ref.shape)


def spread_kernel(parts_ref, out_ref):
    total = jnp.sum(parts_ref[...], axis=0)
    out_ref[...] = jnp.broadcast_to(total[None], out_ref.shape)


def project_kernel(residual_ref, block_hi_ref, block_lo_ref, vectors_ref, out_ref):
    residual = jnp.concatenate([residual_ref[h] for h in range(residual_ref.shape[0])], axis=1)
    rows = residual.shape[0]
    both = jnp.concatenate(split(residual), axis=0)
    along = mxu(both, block_hi_ref[...], NT) + mxu(both, block_lo_ref[...], NT)
    along = along[:rows] + along[rows:]
    projection = dot_f32(along, vectors_ref[...], NN)
    out_ref[...] = jnp.broadcast_to(projection[None], out_ref.shape)


def correct_kernel(parts_ref, scales_ref, vectors_ref, out_ref):
    projection = jnp.sum(parts_ref[...], axis=0) * scales_ref[...]
    out_ref[...] = dot_f32(projection, vectors_ref[...], NT)


def call(kernel, out, *args, **kwargs):
    return pl.pallas_call(
        kernel,
        out_shape=out,
        compiler_params=pltpu.CompilerParams(vmem_limit_bytes=VMEM_LIMIT),
        **kwargs,
    )(*args)


def shape(dims, dtype=jnp.float32):
    return jax.ShapeDtypeStruct(dims, dtype)


def local_part(first, core, centres, mine, other, weights, nystrom_index):
    count, depth = centres.shape
    plane, half, _ = mine.shape
    outputs = weights.shape[0]
    block = nystrom_index.shape[0]
    smem = pl.BlockSpec(memory_space=pltpu.SMEM)
    vmem = pl.BlockSpec(memory_space=pltpu.VMEM)
    anywhere = pl.BlockSpec(memory_space=pl.ANY)
    prepared = call(
        prepare_kernel,
        (
            shape((count, 128)),
            shape((block, depth), jnp.bfloat16),
            shape((block, 128)),
            shape((outputs, count), jnp.bfloat16),
            shape((outputs, count), jnp.bfloat16),
        ),
        first, nystrom_index, centres, weights,
        in_specs=[smem, anywhere, vmem, vmem],
        out_specs=(vmem,) * 5,
        scratch_shapes=[pltpu.SMEM((block,), jnp.int32), pltpu.SemaphoreType.DMA(())],
    )
    norm, points, point_norm, w_hi, w_lo = prepared
    rows_spec = pl.BlockSpec((2, half, depth), lambda i: (i, 0, 0))
    batch = plane * 128
    return call(
        tile_kernel,
        (
            shape((plane, outputs, 128)),
            shape((block, batch), jnp.bfloat16),
            shape((block, batch), jnp.bfloat16),
        ),
        core, mine, other, centres, norm, w_hi, w_lo, points, point_norm,
        grid=(plane // 2,),
        in_specs=[smem, rows_spec, rows_spec] + [vmem] * 6,
        out_specs=(
            pl.BlockSpec((2, outputs, 128), lambda i: (i, 0, 0)),
            pl.BlockSpec((block, 256), lambda i: (0, i)),
            pl.BlockSpec((block, 256), lambda i: (0, i)),
        ),
    )


def exchange(x, axes):
    return lax.all_to_all(x, axes, split_axis=0, concat_axis=0, tiled=True)


def on_device(centres, weights, targets, batch_index, nystrom_index, eigvecs, scales):
    count, depth = centres.shape
    outputs = weights.shape[0]
    own = batch_index.shape[0]
    block = nystrom_index.shape[0]
    anywhere = pl.BlockSpec(memory_space=pl.ANY)
    sizes = {a: lax.axis_size(a) for a in ALL}
    plane = sizes["x"] * sizes["y"]
    column = sizes["z"] * sizes["c"]
    first = (lax.axis_index(ALL) * count).astype(jnp.int32).reshape(1)
    core = lax.axis_index("c").astype(jnp.int32).reshape(1)
    place = lax.axis_index("c") * sizes["z"] + lax.axis_index("z")
    smem = pl.BlockSpec(memory_space=pltpu.SMEM)
    vmem = pl.BlockSpec(memory_space=pltpu.VMEM)

    rows = call(
        pick_kernel,
        shape((sizes["z"], own, depth), jnp.bfloat16),
        first, batch_index, centres,
        in_specs=[smem, anywhere, anywhere],
        out_specs=vmem,
        scratch_shapes=[
            pltpu.SMEM((own,), jnp.int32),
            pltpu.VMEM((own, 8, depth), jnp.bfloat16),
            pltpu.SemaphoreType.DMA(()),
            pltpu.SemaphoreType.DMA((own,)),
        ],
    )
    rows = exchange(rows, ("z",)).reshape(1, sizes["z"] * own, depth)
    mine = exchange(jnp.broadcast_to(rows, (plane, *rows.shape[1:])), PLANE)
    other = lax.ppermute(mine, "c", [(0, 1), (1, 0)])
    predicted, block_hi, block_lo = local_part(
        first, core, centres, mine, other, weights, nystrom_index
    )
    lanes = lax.broadcasted_iota(jnp.int32, (outputs, 128), 1) // own
    less = jnp.where(lanes == place, jnp.tile(targets, (1, 128 // own)), 0.0)
    gathered = exchange(predicted, PLANE)
    summed = call(combine_kernel, shape((column, outputs, 128)), gathered, less)
    summed = exchange(summed, COLUMN)
    residual = call(spread_kernel, shape((plane, outputs, 128)), summed)
    residual_local = lax.dynamic_slice(residual, (0, 0, place * own), (1, outputs, own))[0]
    residual = exchange(residual, PLANE)
    projection = call(
        project_kernel, shape((plane, outputs, 128)), residual, block_hi, block_lo, eigvecs
    )
    projection = exchange(projection, PLANE)
    projection = call(spread_kernel, shape((column, outputs, 128)), projection)
    projection = exchange(projection, COLUMN)
    correction = call(
        correct_kernel, shape((outputs, block)), projection, scales[None, :], eigvecs
    )
    return residual_local, correction


def solution(mesh):
    finer = Mesh(mesh.devices.reshape(mesh.shape["gx"], 4, 4, 2), ALL)
    in_specs = (
        P(ALL, None),
        P(None, ALL),
        P(None, ALL),
        P(ALL),
        P(ALL),
        P(ALL, None),
        P(),
    )
    out_specs = (P(None, ALL), P(None, ALL))
    return jax.shard_map(
        on_device, mesh=finer, in_specs=in_specs, out_specs=out_specs, check_vma=False
    )
```

```python
import math

import jax
import jax.numpy as jnp
from jax import lax
from jax.experimental import pallas as pl
from jax.experimental.pallas import tpu as pltpu
from jax.sharding import Mesh
from jax.sharding import PartitionSpec as P


ALL = ("z", "x", "y", "c")
PLANE = ("x", "y")
COLUMN = ("z", "c")
CHUNK = 256
NT = (((1,), (1,)), ((), ()))
NN = (((1,), (0,)), ((), ()))
VMEM_LIMIT = 24 * 1024 * 1024


def split(v):
    hi = v.astype(jnp.bfloat16)
    lo = (v - hi.astype(jnp.float32)).astype(jnp.bfloat16)
    return hi, lo


def mxu(a, b, dims):
    return lax.dot_general(a, b, dims, preferred_element_type=jnp.float32)


def dot_f32(a, b, dims):
    rows = a.shape[0]
    both = jnp.concatenate(split(a), axis=0)
    b_hi, b_lo = split(b)
    out = mxu(both, b_hi, dims) + mxu(both, b_lo, dims)
    return out[:rows] + out[rows:]


def squares(v):
    wide = v.astype(jnp.float32)
    return split(wide * wide)


def pick_kernel(first_ref, batch_ref, centres_ref, rows_ref, index_ref, tiles_ref, index_sem, sems):
    own = batch_ref.shape[0]
    fetch = pltpu.make_async_copy(batch_ref, index_ref, index_sem)
    fetch.start()
    fetch.wait()
    first = first_ref[0]
    copies = []
    for r in range(own):
        row = index_ref[r] - first
        base = pl.multiple_of((row // 8) * 8, 8)
        copy = pltpu.make_async_copy(
            centres_ref.at[pl.ds(base, 8), :], tiles_ref.at[r], sems.at[r]
        )
        copy.start()
        copies.append(copy)
    sub = lax.broadcasted_iota(jnp.int32, tiles_ref.shape[1:], 0)
    picked = jnp.zeros(tiles_ref.shape[1:], jnp.float32)
    for r, copy in enumerate(copies):
        copy.wait()
        wanted = (index_ref[r] - first) % 8
        tile = jnp.where(sub == wanted, tiles_ref[r].astype(jnp.float32), 0.0)
        picked = jnp.where(sub == r, jnp.sum(tile, axis=0, keepdims=True), picked)
    rows_ref[...] = jnp.broadcast_to(picked.astype(jnp.bfloat16)[None], rows_ref.shape)


def norms(v):
    ones = jnp.ones((v.shape[1], 128), jnp.bfloat16)
    hi, lo = squares(v)
    return mxu(hi, ones, NN) + mxu(lo, ones, NN)


def points_kernel(
    first_ref, block_ref, centres_ref, points_ref, point_norm_ref, index_ref, index_sem
):
    fetch = pltpu.make_async_copy(block_ref, index_ref, index_sem)
    fetch.start()
    fetch.wait()
    first = first_ref[0]
    sub = lax.broadcasted_iota(jnp.int32, (8, 128), 0)
    lane = lax.broadcasted_iota(jnp.int32, (8, 128), 1)
    groups = []
    for start in range(0, points_ref.shape[0], 8):
        tile = jnp.zeros((8, 128), jnp.int32)
        for r in range(8):
            tile = jnp.where(sub == r, index_ref[start + r] - first, tile)
        groups.append(tile)
    found = jnp.zeros(points_ref.shape, jnp.float32)
    for base in range(0, centres_ref.shape[0], 256):
        pieces = []
        for tile in groups:
            halves = [jnp.where(tile == lane + (base + k), 1.0, 0.0) for k in (0, 128)]
            pieces.append(jnp.concatenate(halves, axis=1))
        hot = jnp.concatenate(pieces, axis=0).astype(jnp.bfloat16)
        found = found + mxu(hot, centres_ref[base : base + 256, :], NN)
    points = found.astype(jnp.bfloat16)
    points_ref[...] = points
    point_norm_ref[...] = norms(points)


def norm_kernel(centres_ref, weights_ref, norm_ref, hi_ref, lo_ref):
    for base in range(0, centres_ref.shape[0], 256):
        norm_ref[base : base + 256, :] = norms(centres_ref[base : base + 256, :])
    hi, lo = split(weights_ref[...])
    hi_ref[...] = hi
    lo_ref[...] = lo


def kernel_of(own_ref, other_ref, spans):
    rows = jnp.concatenate([ref[h] for h in spans for ref in (own_ref, other_ref)], axis=0)
    depth = rows.shape[1]
    hi, lo = squares(rows)
    ones = jnp.ones((8, depth), jnp.bfloat16)
    row_norm = (mxu(ones, hi, NT) + mxu(ones, lo, NT))[:1]
    doubled = rows * jnp.bfloat16(-2.0)
    factor = -1.0 / (float(depth) ** 0.5 * math.log(2.0))

    def kernel_values(v, v_norm):
        wide = jnp.concatenate([v_norm] * (rows.shape[0] // 128), axis=1)
        squared = jnp.maximum((wide + row_norm) + mxu(v, doubled, NT), 1.0)
        return jnp.exp2(squared * lax.rsqrt(squared) * factor)

    return kernel_values


def ordered(v, core):
    return jnp.where(core == 1, pltpu.roll(v, 64, 1), v)


def mixed_kernel(
    core_ref, own_ref, other_ref, points_ref, point_norm_ref, vectors_ref, out_ref
):
    e_hi, e_lo = split(vectors_ref[...].T)
    left = jnp.concatenate([e_hi, e_lo, e_hi], axis=1)
    for h in range(0, own_ref.shape[0], 2):
        block = kernel_of(own_ref, other_ref, range(h, h + 2))(points_ref[...], point_norm_ref[...])
        b_hi, b_lo = split(block)
        mixed = mxu(left, jnp.concatenate([b_hi, b_hi, b_lo], axis=0), NN)
        for k in range(2):
            out_ref[h + k] = ordered(mixed[:, k * 128 : (k + 1) * 128], core_ref[0])


def tile_kernel(
    core_ref, own_ref, other_ref, centres_ref, norm_ref, hi_ref, lo_ref, out_ref,
):
    kernel_values = kernel_of(own_ref, other_ref, range(2))
    both_terms = jnp.concatenate([hi_ref[...], lo_ref[...]], axis=0)
    outputs = hi_ref.shape[0]
    total = jnp.zeros((2 * outputs, 4 * own_ref.shape[1]), jnp.float32)
    for base in range(0, centres_ref.shape[0], CHUNK):
        values = kernel_values(
            centres_ref[base : base + CHUNK, :], norm_ref[base : base + CHUNK, :]
        )
        k_hi = values.astype(jnp.bfloat16)
        rest = values - k_hi.astype(jnp.float32)
        terms = both_terms[:, base : base + CHUNK]
        total = total + mxu(terms, k_hi, NN)
        total = total + mxu(terms, rest.astype(jnp.bfloat16), NN)
    predicted = total[:outputs] + total[outputs:]
    for h in range(2):
        out_ref[h] = ordered(predicted[:, h * 128 : (h + 1) * 128], core_ref[0])


def combine_kernel(parts_ref, less_ref, out_ref):
    total = jnp.sum(parts_ref[...], axis=0) - less_ref[...]
    out_ref[...] = jnp.broadcast_to(total[None], out_ref.shape)


def spread_kernel(parts_ref, out_ref):
    total = jnp.sum(parts_ref[...], axis=0)
    out_ref[...] = jnp.broadcast_to(total[None], out_ref.shape)


def project_kernel(parts_ref, mixed_ref, residual_ref, out_ref):
    residual = jnp.sum(parts_ref[...], axis=0)
    residual_ref[...] = residual
    projection = dot_f32(residual, jnp.sum(mixed_ref[...], axis=0), NT)
    out_ref[...] = jnp.broadcast_to(projection[None], out_ref.shape)


def correct_kernel(parts_ref, scales_ref, vectors_ref, out_ref):
    projection = jnp.sum(parts_ref[...], axis=0) * scales_ref[...]
    out_ref[...] = dot_f32(projection, vectors_ref[...], NT)


def call(kernel, out, *args, **kwargs):
    return pl.pallas_call(
        kernel,
        out_shape=out,
        compiler_params=pltpu.CompilerParams(vmem_limit_bytes=VMEM_LIMIT),
        **kwargs,
    )(*args)


def shape(dims, dtype=jnp.float32):
    return jax.ShapeDtypeStruct(dims, dtype)


def local_part(first, core, centres, mine, other, weights, nystrom_index, eigvecs, move):
    count, depth = centres.shape
    plane, half, _ = mine.shape
    outputs = weights.shape[0]
    block = nystrom_index.shape[0]
    eigen = eigvecs.shape[1]
    smem = pl.BlockSpec(memory_space=pltpu.SMEM)
    vmem = pl.BlockSpec(memory_space=pltpu.VMEM)
    stay = pl.BlockSpec(memory_space=pltpu.HBM)
    points, point_norm = call(
        points_kernel,
        (shape((block, depth), jnp.bfloat16), shape((block, 128))),
        first, keep(nystrom_index), centres,
        in_specs=[smem, stay, vmem],
        out_specs=(vmem,) * 2,
        scratch_shapes=[pltpu.SMEM((block,), jnp.int32), pltpu.SemaphoreType.DMA(())],
    )
    mixed = call(
        mixed_kernel, shape((plane, eigen, 128)),
        core, mine, other, points, point_norm, eigvecs,
        in_specs=[smem] + [vmem] * 5,
        out_specs=vmem,
    )
    mixed = move(mixed)
    norm, w_hi, w_lo = call(
        norm_kernel,
        (
            shape((count, 128)),
            shape((outputs, count), jnp.bfloat16),
            shape((outputs, count), jnp.bfloat16),
        ),
        centres, weights,
        in_specs=[vmem] * 2,
        out_specs=(vmem,) * 3,
    )
    rows_spec = pl.BlockSpec((2, half, depth), lambda i: (i, 0, 0))
    predicted = call(
        tile_kernel, shape((plane, outputs, 128)),
        core, mine, other, centres, norm, w_hi, w_lo,
        grid=(plane // 2,),
        in_specs=[smem, rows_spec, rows_spec] + [vmem] * 4,
        out_specs=pl.BlockSpec((2, outputs, 128), lambda i: (i, 0, 0)),
        cost_estimate=pl.CostEstimate(
            flops=3 * 2 * count * 2 * plane * half * depth,
            transcendentals=2 * count * 2 * plane * half,
            bytes_accessed=8 * count * depth,
        ),
    )
    return lax.optimization_barrier((predicted, mixed))


def keep(x):
    return pltpu.with_memory_space_constraint(x, pltpu.HBM)


def exchange(x, axes):
    return lax.all_to_all(x, axes, split_axis=0, concat_axis=0, tiled=True)


def on_device(centres, weights, targets, batch_index, nystrom_index, eigvecs, scales):
    count, depth = centres.shape
    outputs = weights.shape[0]
    own = batch_index.shape[0]
    block = nystrom_index.shape[0]
    stay = pl.BlockSpec(memory_space=pltpu.HBM)
    sizes = {a: lax.axis_size(a) for a in ALL}
    plane = sizes["x"] * sizes["y"]
    column = sizes["z"] * sizes["c"]
    first = (lax.axis_index(ALL) * count).astype(jnp.int32).reshape(1)
    core = lax.axis_index("c").astype(jnp.int32).reshape(1)
    place = lax.axis_index("c") * sizes["z"] + lax.axis_index("z")
    smem = pl.BlockSpec(memory_space=pltpu.SMEM)
    vmem = pl.BlockSpec(memory_space=pltpu.VMEM)

    rows = call(
        pick_kernel,
        shape((sizes["z"], own, depth), jnp.bfloat16),
        first, keep(batch_index), keep(centres),
        in_specs=[smem, stay, stay],
        out_specs=vmem,
        scratch_shapes=[
            pltpu.SMEM((own,), jnp.int32),
            pltpu.VMEM((own, 8, depth), jnp.bfloat16),
            pltpu.SemaphoreType.DMA(()),
            pltpu.SemaphoreType.DMA((own,)),
        ],
    )
    rows = exchange(rows, ("z",)).reshape(1, sizes["z"] * own, depth)
    mine = exchange(jnp.broadcast_to(rows, (plane, *rows.shape[1:])), PLANE)
    other = lax.ppermute(mine, "c", [(0, 1), (1, 0)])
    predicted, mixed = local_part(
        first, core, centres, mine, other, weights, nystrom_index, eigvecs,
        lambda v: exchange(v, PLANE),
    )
    lanes = lax.broadcasted_iota(jnp.int32, (outputs, 128), 1) // own
    less = jnp.where(lanes == place, jnp.tile(targets, (1, 128 // own)), 0.0)
    gathered = exchange(predicted, PLANE)
    summed = call(combine_kernel, shape((column, outputs, 128)), gathered, less)
    summed = exchange(summed, COLUMN)
    residual, projection = call(
        project_kernel,
        (shape((outputs, 128)), shape((plane, outputs, 128))),
        summed, mixed,
    )
    residual_local = lax.dynamic_slice(residual, (0, place * own), (outputs, own))
    projection = exchange(projection, PLANE)
    projection = call(spread_kernel, shape((column, outputs, 128)), projection)
    projection = exchange(projection, COLUMN)
    correction = call(
        correct_kernel, shape((outputs, block)), projection, scales[None, :], eigvecs
    )
    return residual_local, correction


def solution(mesh):
    finer = Mesh(mesh.devices.reshape(mesh.shape["gx"], 4, 4, 2), ALL)
    in_specs = (
        P(ALL, None),
        P(None, ALL),
        P(None, ALL),
        P(ALL),
        P(ALL),
        P(ALL, None),
        P(),
    )
    out_specs = (P(None, ALL), P(None, ALL))
    return jax.shard_map(
        on_device, mesh=finer, in_specs=in_specs, out_specs=out_specs, check_vma=False
    )
```

```python
import math

import jax
import jax.numpy as jnp
from jax import lax
from jax.experimental import pallas as pl
from jax.experimental.pallas import tpu as pltpu
from jax.sharding import Mesh
from jax.sharding import PartitionSpec as P


ALL = ("z", "x", "y", "c")
PLANE = ("x", "y")
COLUMN = ("z", "c")
CHUNK = 256
PER_STEP = 8
NT = (((1,), (1,)), ((), ()))
NN = (((1,), (0,)), ((), ()))
VMEM_LIMIT = 24 * 1024 * 1024


def split(v):
    hi = v.astype(jnp.bfloat16)
    lo = (v - hi.astype(jnp.float32)).astype(jnp.bfloat16)
    return hi, lo


def mxu(a, b, dims):
    return lax.dot_general(a, b, dims, preferred_element_type=jnp.float32)


def dot_f32(a, b, dims):
    rows = a.shape[0]
    both = jnp.concatenate(split(a), axis=0)
    b_hi, b_lo = split(b)
    out = mxu(both, b_hi, dims) + mxu(both, b_lo, dims)
    return out[:rows] + out[rows:]


def squares(v):
    wide = v.astype(jnp.float32)
    return split(wide * wide)


def pick_kernel(first_ref, batch_ref, centres_ref, rows_ref, index_ref, tiles_ref, index_sem, sems):
    own = batch_ref.shape[0]
    fetch = pltpu.make_async_copy(batch_ref, index_ref, index_sem)
    fetch.start()
    fetch.wait()
    first = first_ref[0]
    copies = []
    for r in range(own):
        row = index_ref[r] - first
        base = pl.multiple_of((row // 8) * 8, 8)
        copy = pltpu.make_async_copy(
            centres_ref.at[pl.ds(base, 8), :], tiles_ref.at[r], sems.at[r]
        )
        copy.start()
        copies.append(copy)
    sub = lax.broadcasted_iota(jnp.int32, tiles_ref.shape[1:], 0)
    picked = jnp.zeros(tiles_ref.shape[1:], jnp.float32)
    for r, copy in enumerate(copies):
        copy.wait()
        wanted = (index_ref[r] - first) % 8
        tile = jnp.where(sub == wanted, tiles_ref[r].astype(jnp.float32), 0.0)
        picked = jnp.where(sub == r, jnp.sum(tile, axis=0, keepdims=True), picked)
    rows_ref[...] = jnp.broadcast_to(picked.astype(jnp.bfloat16)[None], rows_ref.shape)


def norms(v):
    ones = jnp.ones((v.shape[1], 128), jnp.bfloat16)
    hi, lo = squares(v)
    return mxu(hi, ones, NN) + mxu(lo, ones, NN)


def points_kernel(
    first_ref, block_ref, centres_ref, points_ref, point_norm_ref, index_ref, index_sem
):
    fetch = pltpu.make_async_copy(block_ref, index_ref, index_sem)
    fetch.start()
    fetch.wait()
    first = first_ref[0]
    sub = lax.broadcasted_iota(jnp.int32, (8, 128), 0)
    lane = lax.broadcasted_iota(jnp.int32, (8, 128), 1)
    groups = []
    for start in range(0, points_ref.shape[0], 8):
        tile = jnp.zeros((8, 128), jnp.int32)
        for r in range(8):
            tile = jnp.where(sub == r, index_ref[start + r] - first, tile)
        groups.append(tile)
    found = jnp.zeros(points_ref.shape, jnp.float32)
    for base in range(0, centres_ref.shape[0], 256):
        pieces = []
        for tile in groups:
            halves = [jnp.where(tile == lane + (base + k), 1.0, 0.0) for k in (0, 128)]
            pieces.append(jnp.concatenate(halves, axis=1))
        hot = jnp.concatenate(pieces, axis=0).astype(jnp.bfloat16)
        found = found + mxu(hot, centres_ref[base : base + 256, :], NN)
    points = found.astype(jnp.bfloat16)
    points_ref[...] = points
    point_norm_ref[...] = norms(points)


def norm_kernel(centres_ref, weights_ref, norm_ref, hi_ref, lo_ref):
    for base in range(0, centres_ref.shape[0], 256):
        norm_ref[base : base + 256, :] = norms(centres_ref[base : base + 256, :])
    hi, lo = split(weights_ref[...])
    hi_ref[...] = hi
    lo_ref[...] = lo


def kernel_of(own_ref, other_ref, spans):
    rows = jnp.concatenate([ref[h] for h in spans for ref in (own_ref, other_ref)], axis=0)
    depth = rows.shape[1]
    hi, lo = squares(rows)
    ones = jnp.ones((8, depth), jnp.bfloat16)
    row_norm = (mxu(ones, hi, NT) + mxu(ones, lo, NT))[:1]
    doubled = rows * jnp.bfloat16(-2.0)
    factor = -1.0 / (float(depth) ** 0.5 * math.log(2.0))

    def kernel_values(v, v_norm):
        wide = jnp.concatenate([v_norm] * (rows.shape[0] // 128), axis=1)
        squared = jnp.maximum((wide + row_norm) + mxu(v, doubled, NT), 1.0)
        return jnp.exp2(squared * lax.rsqrt(squared) * factor)

    return kernel_values


def ordered(v, core):
    return jnp.where(core == 1, pltpu.roll(v, 64, 1), v)


def mixed_kernel(
    core_ref, own_ref, other_ref, points_ref, point_norm_ref, vectors_ref, out_ref
):
    e_hi, e_lo = split(vectors_ref[...].T)
    left = jnp.concatenate([e_hi, e_lo, e_hi], axis=1)
    for h in range(0, own_ref.shape[0], 2):
        block = kernel_of(own_ref, other_ref, range(h, h + 2))(points_ref[...], point_norm_ref[...])
        b_hi, b_lo = split(block)
        mixed = mxu(left, jnp.concatenate([b_hi, b_hi, b_lo], axis=0), NN)
        for k in range(2):
            out_ref[h + k] = ordered(mixed[:, k * 128 : (k + 1) * 128], core_ref[0])


def tile_kernel(
    core_ref, own_ref, other_ref, centres_ref, norm_ref, hi_ref, lo_ref, out_ref,
):
    both_terms = jnp.concatenate([hi_ref[...], lo_ref[...]], axis=0)
    outputs = hi_ref.shape[0]

    def step(start):
        own_part = own_ref[pl.ds(start, PER_STEP)]
        other_part = other_ref[pl.ds(start, PER_STEP)]
        makers = [
            kernel_of(own_part, other_part, range(h, h + 2)) for h in range(0, PER_STEP, 2)
        ]
        for p, kernel_values in enumerate(makers):
            total = jnp.zeros((2 * outputs, 4 * own_ref.shape[1]), jnp.float32)
            for base in range(0, centres_ref.shape[0], CHUNK):
                values = kernel_values(
                    centres_ref[base : base + CHUNK, :], norm_ref[base : base + CHUNK, :]
                )
                k_hi, k_lo = split(values)
                terms = both_terms[:, base : base + CHUNK]
                total = total + mxu(terms, k_hi, NN)
                total = total + mxu(terms, k_lo, NN)
            predicted = total[:outputs] + total[outputs:]
            for k in range(2):
                part = ordered(predicted[:, k * 128 : (k + 1) * 128], core_ref[0])
                out_ref[start + 2 * p + k] = part

    step(0)


def combine_kernel(parts_ref, less_ref, out_ref):
    total = jnp.sum(parts_ref[...], axis=0) - less_ref[...]
    out_ref[...] = jnp.broadcast_to(total[None], out_ref.shape)


def spread_kernel(parts_ref, out_ref):
    total = jnp.sum(parts_ref[...], axis=0)
    out_ref[...] = jnp.broadcast_to(total[None], out_ref.shape)


def project_kernel(place_ref, parts_ref, mixed_ref, local_ref, out_ref, turned_ref):
    residual = jnp.sum(parts_ref[...], axis=0)
    own = local_ref.shape[0]
    turned_ref[...] = residual.T
    local_ref[...] = turned_ref[pl.ds(pl.multiple_of(place_ref[0] * own, own), own), :]
    projection = dot_f32(residual, jnp.sum(mixed_ref[...], axis=0), NT)
    out_ref[...] = jnp.broadcast_to(projection[None], out_ref.shape)


def correct_kernel(parts_ref, scales_ref, vectors_ref, out_ref):
    projection = jnp.sum(parts_ref[...], axis=0) * scales_ref[...]
    out_ref[...] = dot_f32(projection, vectors_ref[...], NT)


def call(kernel, out, *args, **kwargs):
    return pl.pallas_call(
        kernel,
        out_shape=out,
        compiler_params=pltpu.CompilerParams(vmem_limit_bytes=VMEM_LIMIT),
        **kwargs,
    )(*args)


def shape(dims, dtype=jnp.float32):
    return jax.ShapeDtypeStruct(dims, dtype)


def local_part(first, core, centres, mine, other, weights, nystrom_index, eigvecs, move):
    count, depth = centres.shape
    plane, half, _ = mine.shape
    outputs = weights.shape[0]
    block = nystrom_index.shape[0]
    eigen = eigvecs.shape[1]
    smem = pl.BlockSpec(memory_space=pltpu.SMEM)
    vmem = pl.BlockSpec(memory_space=pltpu.VMEM)
    stay = pl.BlockSpec(memory_space=pltpu.HBM)
    points, point_norm = call(
        points_kernel,
        (shape((block, depth), jnp.bfloat16), shape((block, 128))),
        first, keep(nystrom_index), centres,
        in_specs=[smem, stay, vmem],
        out_specs=(vmem,) * 2,
        scratch_shapes=[pltpu.SMEM((block,), jnp.int32), pltpu.SemaphoreType.DMA(())],
    )
    mixed = call(
        mixed_kernel, shape((plane, eigen, 128)),
        core, mine, other, points, point_norm, eigvecs,
        in_specs=[smem] + [vmem] * 5,
        out_specs=vmem,
    )
    mixed = move(mixed)
    norm, w_hi, w_lo = call(
        norm_kernel,
        (
            shape((count, 128)),
            shape((outputs, count), jnp.bfloat16),
            shape((outputs, count), jnp.bfloat16),
        ),
        centres, weights,
        in_specs=[vmem] * 2,
        out_specs=(vmem,) * 3,
    )
    rows_spec = pl.BlockSpec((PER_STEP, half, depth), lambda i: (i, 0, 0))
    predicted = call(
        tile_kernel, shape((plane, outputs, 128)),
        core, mine, other, centres, norm, w_hi, w_lo,
        grid=(plane // PER_STEP,),
        in_specs=[smem, rows_spec, rows_spec] + [vmem] * 4,
        out_specs=pl.BlockSpec((PER_STEP, outputs, 128), lambda i: (i, 0, 0)),
        cost_estimate=pl.CostEstimate(
            flops=3 * 2 * count * 2 * plane * half * depth,
            transcendentals=2 * count * 2 * plane * half,
            bytes_accessed=8 * count * depth,
        ),
    )
    return lax.optimization_barrier((predicted, mixed))


def keep(x):
    return pltpu.with_memory_space_constraint(x, pltpu.HBM)


def exchange(x, axes):
    return lax.all_to_all(x, axes, split_axis=0, concat_axis=0, tiled=True)


def on_device(centres, weights, targets, batch_index, nystrom_index, eigvecs, scales):
    count, depth = centres.shape
    outputs = weights.shape[0]
    own = batch_index.shape[0]
    block = nystrom_index.shape[0]
    stay = pl.BlockSpec(memory_space=pltpu.HBM)
    sizes = {a: lax.axis_size(a) for a in ALL}
    plane = sizes["x"] * sizes["y"]
    column = sizes["z"] * sizes["c"]
    first = (lax.axis_index(ALL) * count).astype(jnp.int32).reshape(1)
    core = lax.axis_index("c").astype(jnp.int32).reshape(1)
    place = lax.axis_index("c") * sizes["z"] + lax.axis_index("z")
    smem = pl.BlockSpec(memory_space=pltpu.SMEM)
    vmem = pl.BlockSpec(memory_space=pltpu.VMEM)

    rows = call(
        pick_kernel,
        shape((sizes["z"], own, depth), jnp.bfloat16),
        first, keep(batch_index), keep(centres),
        in_specs=[smem, stay, stay],
        out_specs=vmem,
        scratch_shapes=[
            pltpu.SMEM((own,), jnp.int32),
            pltpu.VMEM((own, 8, depth), jnp.bfloat16),
            pltpu.SemaphoreType.DMA(()),
            pltpu.SemaphoreType.DMA((own,)),
        ],
    )
    rows = exchange(rows, ("z",)).reshape(1, sizes["z"] * own, depth)
    mine = exchange(jnp.broadcast_to(rows, (plane, *rows.shape[1:])), PLANE)
    other = lax.ppermute(mine, "c", [(0, 1), (1, 0)])
    predicted, mixed = local_part(
        first, core, centres, mine, other, weights, nystrom_index, eigvecs,
        lambda v: exchange(v, PLANE),
    )
    lanes = lax.broadcasted_iota(jnp.int32, (outputs, 128), 1) // own
    less = jnp.where(lanes == place, jnp.tile(targets, (1, 128 // own)), 0.0)
    gathered = exchange(predicted, PLANE)
    summed = call(combine_kernel, shape((column, outputs, 128)), gathered, less)
    summed = exchange(summed, COLUMN)
    residual, projection = call(
        project_kernel,
        (shape((own, outputs)), shape((plane, outputs, 128))),
        place.astype(jnp.int32).reshape(1), summed, mixed,
        in_specs=[smem, vmem, vmem],
        out_specs=(vmem, vmem),
        scratch_shapes=[pltpu.VMEM((128, outputs), jnp.float32)],
    )
    projection = exchange(projection, PLANE)
    projection = call(spread_kernel, shape((column, outputs, 128)), projection)
    projection = exchange(projection, COLUMN)
    correction = call(
        correct_kernel, shape((outputs, block)), projection, scales[None, :], eigvecs
    )
    return residual.T, correction


def solution(mesh):
    finer = Mesh(mesh.devices.reshape(mesh.shape["gx"], 4, 4, 2), ALL)
    in_specs = (
        P(ALL, None),
        P(None, ALL),
        P(None, ALL),
        P(ALL),
        P(ALL),
        P(ALL, None),
        P(),
    )
    out_specs = (P(None, ALL), P(None, ALL))
    return jax.shard_map(
        on_device, mesh=finer, in_specs=in_specs, out_specs=out_specs, check_vma=False
    )
```

```python
import math

import jax
import jax.numpy as jnp
from jax import lax
from jax.experimental import pallas as pl
from jax.experimental.pallas import tpu as pltpu
from jax.sharding import Mesh
from jax.sharding import PartitionSpec as P


ALL = ("z", "x", "y", "c")
PLANE = ("x", "y")
COLUMN = ("z", "c")
CHUNK = 256
PER_STEP = 8
NT = (((1,), (1,)), ((), ()))
NN = (((1,), (0,)), ((), ()))
VMEM_LIMIT = 24 * 1024 * 1024


def split(v):
    hi = v.astype(jnp.bfloat16)
    lo = (v - hi.astype(jnp.float32)).astype(jnp.bfloat16)
    return hi, lo


def mxu(a, b, dims):
    return lax.dot_general(a, b, dims, preferred_element_type=jnp.float32)


def dot_f32(a, b, dims):
    rows = a.shape[0]
    both = jnp.concatenate(split(a), axis=0)
    b_hi, b_lo = split(b)
    out = mxu(both, b_hi, dims) + mxu(both, b_lo, dims)
    return out[:rows] + out[rows:]


def squares(v):
    wide = v.astype(jnp.float32)
    return split(wide * wide)


def pick_kernel(first_ref, batch_ref, centres_ref, rows_ref, index_ref, tiles_ref, index_sem, sems):
    own = batch_ref.shape[0]
    fetch = pltpu.make_async_copy(batch_ref, index_ref, index_sem)
    fetch.start()
    fetch.wait()
    first = first_ref[0]
    copies = []
    for r in range(own):
        row = index_ref[r] - first
        base = pl.multiple_of((row // 8) * 8, 8)
        copy = pltpu.make_async_copy(
            centres_ref.at[pl.ds(base, 8), :], tiles_ref.at[r], sems.at[r]
        )
        copy.start()
        copies.append(copy)
    sub = lax.broadcasted_iota(jnp.int32, tiles_ref.shape[1:], 0)
    picked = jnp.zeros(tiles_ref.shape[1:], jnp.float32)
    for r, copy in enumerate(copies):
        copy.wait()
        wanted = (index_ref[r] - first) % 8
        tile = jnp.where(sub == wanted, tiles_ref[r].astype(jnp.float32), 0.0)
        picked = jnp.where(sub == r, jnp.sum(tile, axis=0, keepdims=True), picked)
    rows_ref[...] = jnp.broadcast_to(picked.astype(jnp.bfloat16)[None], rows_ref.shape)


def norms(v):
    ones = jnp.ones((v.shape[1], 128), jnp.bfloat16)
    hi, lo = squares(v)
    return mxu(hi, ones, NN) + mxu(lo, ones, NN)


def points_kernel(
    first_ref, block_ref, centres_ref, points_ref, point_norm_ref, index_ref, index_sem
):
    fetch = pltpu.make_async_copy(block_ref, index_ref, index_sem)
    fetch.start()
    fetch.wait()
    first = first_ref[0]
    sub = lax.broadcasted_iota(jnp.int32, (8, 128), 0)
    lane = lax.broadcasted_iota(jnp.int32, (8, 128), 1)
    groups = []
    for start in range(0, points_ref.shape[0], 8):
        tile = jnp.zeros((8, 128), jnp.int32)
        for r in range(8):
            tile = jnp.where(sub == r, index_ref[start + r] - first, tile)
        groups.append(tile)
    found = jnp.zeros(points_ref.shape, jnp.float32)
    for base in range(0, centres_ref.shape[0], 256):
        pieces = []
        for tile in groups:
            halves = [jnp.where(tile == lane + (base + k), 1.0, 0.0) for k in (0, 128)]
            pieces.append(jnp.concatenate(halves, axis=1))
        hot = jnp.concatenate(pieces, axis=0).astype(jnp.bfloat16)
        found = found + mxu(hot, centres_ref[base : base + 256, :], NN)
    points = found.astype(jnp.bfloat16)
    points_ref[...] = points
    point_norm_ref[...] = norms(points)


def norm_kernel(centres_ref, weights_ref, norm_ref, hi_ref, lo_ref):
    for base in range(0, centres_ref.shape[0], 256):
        norm_ref[base : base + 256, :] = norms(centres_ref[base : base + 256, :])
    hi, lo = split(weights_ref[...])
    hi_ref[...] = hi
    lo_ref[...] = lo


def kernel_of(own_ref, other_ref, spans):
    rows = jnp.concatenate([ref[h] for h in spans for ref in (own_ref, other_ref)], axis=0)
    depth = rows.shape[1]
    hi, lo = squares(rows)
    ones = jnp.ones((8, depth), jnp.bfloat16)
    row_norm = (mxu(ones, hi, NT) + mxu(ones, lo, NT))[:1]
    doubled = rows * jnp.bfloat16(-2.0)
    factor = -1.0 / (float(depth) ** 0.5 * math.log(2.0))

    def kernel_values(v, v_norm):
        wide = jnp.concatenate([v_norm] * (rows.shape[0] // 128), axis=1)
        squared = jnp.maximum((wide + row_norm) + mxu(v, doubled, NT), 1.0)
        return jnp.exp2(squared * lax.rsqrt(squared) * factor)

    return kernel_values


def ordered(v, core):
    return jnp.where(core == 1, pltpu.roll(v, 64, 1), v)


def mixed_kernel(
    core_ref, own_ref, other_ref, points_ref, point_norm_ref, vectors_ref, out_ref
):
    e_hi, e_lo = split(vectors_ref[...].T)
    left = jnp.concatenate([e_hi, e_lo, e_hi], axis=1)
    for h in range(0, own_ref.shape[0], 2):
        block = kernel_of(own_ref, other_ref, range(h, h + 2))(points_ref[...], point_norm_ref[...])
        b_hi, b_lo = split(block)
        mixed = mxu(left, jnp.concatenate([b_hi, b_hi, b_lo], axis=0), NN)
        for k in range(2):
            out_ref[h + k] = ordered(mixed[:, k * 128 : (k + 1) * 128], core_ref[0])


def tile_kernel(
    core_ref, own_ref, other_ref, centres_ref, norm_ref, hi_ref, lo_ref, out_ref,
):
    both_terms = jnp.concatenate([hi_ref[...], lo_ref[...]], axis=0)
    outputs = hi_ref.shape[0]

    def step(start):
        own_part = own_ref[pl.ds(start, PER_STEP)]
        other_part = other_ref[pl.ds(start, PER_STEP)]
        makers = [
            kernel_of(own_part, other_part, range(h, h + 2)) for h in range(0, PER_STEP, 2)
        ]
        for p, kernel_values in enumerate(makers):
            total = jnp.zeros((2 * outputs, 4 * own_ref.shape[1]), jnp.float32)
            for base in range(0, centres_ref.shape[0], CHUNK):
                values = kernel_values(
                    centres_ref[base : base + CHUNK, :], norm_ref[base : base + CHUNK, :]
                )
                k_hi, k_lo = split(values)
                terms = both_terms[:, base : base + CHUNK]
                total = total + mxu(terms, k_hi, NN)
                total = total + mxu(terms, k_lo, NN)
            predicted = total[:outputs] + total[outputs:]
            for k in range(2):
                part = ordered(predicted[:, k * 128 : (k + 1) * 128], core_ref[0])
                out_ref[start + 2 * p + k] = part

    step(0)


def combine_kernel(parts_ref, less_ref, out_ref):
    total = jnp.sum(parts_ref[...], axis=0) - less_ref[...]
    out_ref[...] = jnp.broadcast_to(total[None], out_ref.shape)


def spread_kernel(parts_ref, out_ref):
    total = jnp.sum(parts_ref[...], axis=0)
    out_ref[...] = jnp.broadcast_to(total[None], out_ref.shape)


def project_kernel(place_ref, parts_ref, mixed_ref, local_ref, out_ref, turned_ref):
    residual = jnp.sum(parts_ref[...], axis=0)
    own = local_ref.shape[0]
    turned_ref[...] = residual.T
    local_ref[...] = turned_ref[pl.ds(pl.multiple_of(place_ref[0] * own, own), own), :]
    projection = dot_f32(residual, jnp.sum(mixed_ref[...], axis=0), NT)
    out_ref[...] = jnp.broadcast_to(projection[None], out_ref.shape)


def correct_kernel(parts_ref, scales_ref, vectors_ref, out_ref):
    projection = jnp.sum(parts_ref[...], axis=0) * scales_ref[...]
    out_ref[...] = dot_f32(projection, vectors_ref[...], NT)


def call(kernel, out, *args, **kwargs):
    return pl.pallas_call(
        kernel,
        out_shape=out,
        compiler_params=pltpu.CompilerParams(vmem_limit_bytes=VMEM_LIMIT),
        **kwargs,
    )(*args)


def shape(dims, dtype=jnp.float32):
    return jax.ShapeDtypeStruct(dims, dtype)


def local_part(first, core, centres, mine, other, weights, nystrom_index, eigvecs, move, less):
    count, depth = centres.shape
    plane, half, _ = mine.shape
    outputs = weights.shape[0]
    block = nystrom_index.shape[0]
    eigen = eigvecs.shape[1]
    smem = pl.BlockSpec(memory_space=pltpu.SMEM)
    vmem = pl.BlockSpec(memory_space=pltpu.VMEM)
    stay = pl.BlockSpec(memory_space=pltpu.HBM)
    points, point_norm = call(
        points_kernel,
        (shape((block, depth), jnp.bfloat16), shape((block, 128))),
        first, keep(nystrom_index), centres,
        in_specs=[smem, stay, vmem],
        out_specs=(vmem,) * 2,
        scratch_shapes=[pltpu.SMEM((block,), jnp.int32), pltpu.SemaphoreType.DMA(())],
    )
    points, less = lax.optimization_barrier((points, less))
    mixed = call(
        mixed_kernel, shape((plane, eigen, 128)),
        core, mine, other, points, point_norm, eigvecs,
        in_specs=[smem] + [vmem] * 5,
        out_specs=vmem,
    )
    mixed = move(mixed)
    norm, w_hi, w_lo = call(
        norm_kernel,
        (
            shape((count, 128)),
            shape((outputs, count), jnp.bfloat16),
            shape((outputs, count), jnp.bfloat16),
        ),
        centres, weights,
        in_specs=[vmem] * 2,
        out_specs=(vmem,) * 3,
    )
    rows_spec = pl.BlockSpec((PER_STEP, half, depth), lambda i: (i, 0, 0))
    predicted = call(
        tile_kernel, shape((plane, outputs, 128)),
        core, mine, other, centres, norm, w_hi, w_lo,
        grid=(plane // PER_STEP,),
        in_specs=[smem, rows_spec, rows_spec] + [vmem] * 4,
        out_specs=pl.BlockSpec((PER_STEP, outputs, 128), lambda i: (i, 0, 0)),
        cost_estimate=pl.CostEstimate(
            flops=3 * 2 * count * 2 * plane * half * depth,
            transcendentals=2 * count * 2 * plane * half,
            bytes_accessed=8 * count * depth,
        ),
    )
    return (*lax.optimization_barrier((predicted, mixed)), less)


def keep(x):
    return pltpu.with_memory_space_constraint(x, pltpu.HBM)


def exchange(x, axes):
    return lax.all_to_all(x, axes, split_axis=0, concat_axis=0, tiled=True)


def on_device(centres, weights, targets, batch_index, nystrom_index, eigvecs, scales):
    count, depth = centres.shape
    outputs = weights.shape[0]
    own = batch_index.shape[0]
    block = nystrom_index.shape[0]
    stay = pl.BlockSpec(memory_space=pltpu.HBM)
    sizes = {a: lax.axis_size(a) for a in ALL}
    plane = sizes["x"] * sizes["y"]
    column = sizes["z"] * sizes["c"]
    first = (lax.axis_index(ALL) * count).astype(jnp.int32).reshape(1)
    core = lax.axis_index("c").astype(jnp.int32).reshape(1)
    place = lax.axis_index("c") * sizes["z"] + lax.axis_index("z")
    smem = pl.BlockSpec(memory_space=pltpu.SMEM)
    vmem = pl.BlockSpec(memory_space=pltpu.VMEM)

    rows = call(
        pick_kernel,
        shape((sizes["z"], own, depth), jnp.bfloat16),
        first, keep(batch_index), keep(centres),
        in_specs=[smem, stay, stay],
        out_specs=vmem,
        scratch_shapes=[
            pltpu.SMEM((own,), jnp.int32),
            pltpu.VMEM((own, 8, depth), jnp.bfloat16),
            pltpu.SemaphoreType.DMA(()),
            pltpu.SemaphoreType.DMA((own,)),
        ],
    )
    rows = exchange(rows, ("z",)).reshape(1, sizes["z"] * own, depth)
    mine = exchange(jnp.broadcast_to(rows, (plane, *rows.shape[1:])), PLANE)
    mine, targets = lax.optimization_barrier((mine, targets))
    lanes = lax.broadcasted_iota(jnp.int32, (outputs, 128), 1) // own
    less = jnp.where(lanes == place, jnp.tile(targets, (1, 128 // own)), 0.0)
    other = lax.ppermute(mine, "c", [(0, 1), (1, 0)])
    predicted, mixed, less = local_part(
        first, core, centres, mine, other, weights, nystrom_index, eigvecs,
        lambda v: exchange(v, PLANE), less,
    )
    gathered = exchange(predicted, PLANE)
    summed = call(combine_kernel, shape((column, outputs, 128)), gathered, less)
    summed = exchange(summed, COLUMN)
    residual, projection = call(
        project_kernel,
        (shape((own, outputs)), shape((plane, outputs, 128))),
        place.astype(jnp.int32).reshape(1), summed, mixed,
        in_specs=[smem, vmem, vmem],
        out_specs=(vmem, vmem),
        scratch_shapes=[pltpu.VMEM((128, outputs), jnp.float32)],
    )
    projection = exchange(projection, PLANE)
    projection = call(spread_kernel, shape((column, outputs, 128)), projection)
    projection = exchange(projection, COLUMN)
    correction = call(
        correct_kernel, shape((outputs, block)), projection, scales[None, :], eigvecs
    )
    return residual.T, correction


def solution(mesh):
    finer = Mesh(mesh.devices.reshape(mesh.shape["gx"], 4, 4, 2), ALL)
    in_specs = (
        P(ALL, None),
        P(None, ALL),
        P(None, ALL),
        P(ALL),
        P(ALL),
        P(ALL, None),
        P(),
    )
    out_specs = (P(None, ALL), P(None, ALL))
    return jax.shard_map(
        on_device, mesh=finer, in_specs=in_specs, out_specs=out_specs, check_vma=False
    )
```
